32 devices in a mesh: silo: 4 (over z), row: 8 (over y, x, core).
Axes of the slice: x: 2, y: 2, z: 4, core: 2. Of those that a mesh axis runs over, the one named last changes fastest.
Arguments:
- silo_grams: float32 [8, 4096, 4096], P('silo', 'row'), may hold values from -9 to 81, as said below
- silo_weights: bfloat16 [8, 4096, 640], P('silo', 'row'), may hold values from -6 to 6
Outputs:
- merged_rows: float32 [640, 4096], P(('silo', 'row'))
The draws below stay inside these ranges and needn't reach their ends.
Inputs may be any that keep to these rules, and one draw needn't show every extreme that they name: `silo_grams`: each silo's Gram is symmetric up to float32 rounding and positive definite.
All inputs are finite; a program needn't handle non-finite values.
Results may differ from the reference program's by a relative error of at most 0.0003.
Values may be sent and summed in bfloat16 or wider, within the bound.
No kernel may reach another device: no remote copies, remote signals or barrier semaphores. Data moves between devices by JAX's collectives and lax.ppermute only.
A program may use at most 128 MiB of HBM per device.

```python
import math
import jax
import jax.numpy as jnp
from jax import lax

D = 4096
C = 640
ITERS = 2
SILOS = 8


def noise_matrix(noise_key):
    raw_noise = jnp.clip(jax.random.normal(noise_key, (D, D), jnp.float32), -4.0, 4.0)
    return (raw_noise + raw_noise.T) * (0.45 / (2.0 * math.sqrt(2.0 * D)))


def draw_silo_grams(key, part):
    key_scale, key_common, key_silos = jax.random.split(jax.random.fold_in(key, 17), 3)
    row_trend = 1.0 + 2.0 * jnp.arange(D, dtype=jnp.float32) / D
    row_scale = row_trend * jnp.exp(jax.random.uniform(key_scale, (D,), jnp.float32, 0.0, math.log(2.0)))
    common_part = noise_matrix(key_common)

    def single_silo(silo_key):
        key_level, key_own = jax.random.split(silo_key)
        silo_level = jax.random.uniform(key_level, (D,), jnp.float32, 1.0, 2.0)
        silo_matrix = common_part + noise_matrix(key_own) + jnp.diag(silo_level)
        return row_scale[:, None] * silo_matrix * row_scale[None, :]
    return lax.map(single_silo, jax.random.split(key_silos, SILOS))


def shard_levels(rng, dims, cuts, least, high):
    factor_of = 1.0
    for dim, shards_of in cuts:
        heights = jax.random.uniform(jax.random.fold_in(jax.random.fold_in(rng, 6), dim), (shards_of,), jnp.float32, least / len(cuts), high / len(cuts))
        factor_of = factor_of * jnp.repeat(jnp.exp(heights), dims[dim] // shards_of).reshape((-1,) + (1,) * (len(dims) - 1 - dim))
    return factor_of


def bell_draw(key, extent, scale, bound, cuts=(), kind=jnp.bfloat16):
    drawn = jax.random.normal(key, extent, jnp.float32) * scale
    if len(cuts) > 0:
        drawn = shard_levels(key, extent, cuts, -0.22, 0.18) * drawn
    return jnp.clip(drawn, min=-bound, max=bound).astype(kind)


def setup_inputs(seed: int = 0) -> dict:
    seeds = jax.random.split(jax.random.key(seed), 3)
    silo_grams = draw_silo_grams(jax.random.fold_in(seeds[2], 71), 0)
    silo_weights = bell_draw(seeds[1], (SILOS, D, C), 1.0, 6.0, ((0, 4), (1, 8)))
    return dict(silo_grams=silo_grams, silo_weights=silo_weights)


full_precision = lax.Precision.HIGHEST

def conj_grad(right_side, operator):
    solution = jnp.zeros_like(right_side)
    residual = right_side
    direction = right_side
    res_norm = lax.optimization_barrier(jnp.sum(residual * residual, axis=0))
    for iteration in range(ITERS):
        mapped = jnp.dot(operator, direction, precision=full_precision)
        step_size = res_norm / lax.optimization_barrier(jnp.sum(direction * mapped, axis=0))
        solution = solution + step_size * direction
        residual = residual - step_size * mapped
        next_norm = lax.optimization_barrier(jnp.sum(residual * residual, axis=0))
        direction = residual + next_norm / res_norm * direction
        res_norm = next_norm
    return solution

def reference(silo_grams, silo_weights):
    operator = lax.optimization_barrier(jnp.sum(silo_grams, axis=0))

    def add_silo(running, paired):
        silo_gram, silo_weight = paired
        return (running + jnp.dot(silo_gram, silo_weight.astype(jnp.float32), precision=full_precision), None)
    right_side, unused = lax.scan(add_silo, jnp.zeros((D, C), jnp.float32), (silo_grams, silo_weights))
    solution = conj_grad(right_side, operator)
    return solution.T
```

```python
import functools

import jax
import jax.numpy as jnp
from jax import lax
from jax.experimental import pallas as pl
from jax.experimental.pallas import tpu as pltpu
from jax.sharding import PartitionSpec as P


f32, bf16, f16 = jnp.float32, jnp.bfloat16, jnp.float16
CHUNKS = 1


def swap(value, axis, size, bit):
    return lax.ppermute(value, axis, [(i, i ^ bit) for i in range(size)])


def split(value):
    high = lax.reduce_precision(value, 8, 7)
    return high.astype(bf16), (value - high).astype(bf16)


def split_here(value):
    high = value.astype(bf16)
    return high, (value - high.astype(f32)).astype(bf16)


def nn(left, right):
    return lax.dot_general(left, right, (((1,), (0,)), ((), ())), preferred_element_type=f32)


def tile_of(rows):
    return 256 if rows % 256 == 0 else rows


def prepare_kernel(row_ref, gram_ref, high_ref, low_ref, sums_ref, diag_ref):
    block = pl.program_id(0)
    rows = gram_ref.shape[1]
    total = jnp.sum(gram_ref[...], axis=0)
    high, low = split_here(total.T)
    high_ref[...] = high
    low_ref[...] = low
    sizes = jnp.sum(jnp.abs(gram_ref[...]), axis=0)

    @pl.when(block == 0)
    def _():
        sums_ref[...] = jnp.zeros_like(sums_ref)

    sums_ref[...] += jnp.sum(sizes, axis=1, keepdims=True)

    @pl.when(block == row_ref[0])
    def _():
        here = lax.broadcasted_iota(jnp.int32, (rows, rows), 0)
        there = lax.broadcasted_iota(jnp.int32, (rows, rows), 1)
        diag_ref[...] = jnp.sum(jnp.where(here == there, total, 0.0), axis=1, keepdims=True)


def prepare(grams, row):
    silos, rows, width = grams.shape
    shape = jax.ShapeDtypeStruct
    return pl.pallas_call(
        prepare_kernel,
        grid_spec=pltpu.PrefetchScalarGridSpec(
            num_scalar_prefetch=1,
            grid=(width // rows,),
            in_specs=[pl.BlockSpec((silos, rows, rows), lambda k, row: (0, 0, k))],
            out_specs=[
                pl.BlockSpec((rows, rows), lambda k, row: (k, 0)),
                pl.BlockSpec((rows, rows), lambda k, row: (k, 0)),
                pl.BlockSpec((rows, 1), lambda k, row: (0, 0)),
                pl.BlockSpec((rows, 1), lambda k, row: (0, 0)),
            ],
        ),
        out_shape=[shape((width, rows), bf16), shape((width, rows), bf16), shape((rows, 1), f32), shape((rows, 1), f32)],
        cost_estimate=pl.CostEstimate(flops=400 * grams.size, bytes_accessed=6 * grams.size, transcendentals=0),
        name="prepare",
    )(row[None], grams)


def rhs_kernel(count, parts, last, where_ref, *refs):
    grams, weights, rest = refs[:count], refs[count : count * (1 + parts)], refs[count * (1 + parts) :]
    out_ref = rest[-1]
    total = rest[0][...] if len(rest) > 1 else None
    for k in range(count):
        tile = grams[k].shape[1]
        each = grams[k].shape[0] // parts
        for i in range(grams[k].shape[0]):
            both = jnp.concatenate(split_here(grams[k][i]), axis=0)
            term = nn(both, weights[k * parts + i // each][i % each])
            term = term[:tile] + term[tile:]
            total = term if total is None else total + term
    out_ref[...] = total.T if last else total


def rhs(pieces, grams, where, total, last):
    silos, rows, _ = grams.shape
    parts = len(pieces[0])
    depth, cols = pieces[0][0].shape[1:]
    tile = tile_of(rows)
    count = len(pieces)
    flat = [half for piece in pieces for half in piece]
    more = [] if total is None else [total]
    in_specs = [pl.BlockSpec((silos, tile, depth), functools.partial(lambda p, r, where: (0, r, where[p]), p)) for p in range(count)]
    in_specs += [pl.BlockSpec(half.shape, lambda r, where: (0, 0, 0)) for half in flat]
    in_specs += [pl.BlockSpec((tile, cols), lambda r, where: (r, 0)) for _ in more]
    return pl.pallas_call(
        functools.partial(rhs_kernel, count, parts, last),
        grid_spec=pltpu.PrefetchScalarGridSpec(
            num_scalar_prefetch=1,
            grid=(rows // tile,),
            in_specs=in_specs,
            out_specs=pl.BlockSpec((cols, tile), lambda r, where: (0, r)) if last else pl.BlockSpec((tile, cols), lambda r, where: (r, 0)),
        ),
        out_shape=jax.ShapeDtypeStruct((cols, rows) if last else (rows, cols), f32),
        cost_estimate=pl.CostEstimate(
            flops=8 * count * silos * rows * depth * cols, bytes_accessed=4 * count * silos * rows * depth, transcendentals=0
        ),
        name="rhs",
    )(where, *([grams] * count), *flat, *more)


def apply_kernel(shape, exact, where_ref, *refs):
    refs = list(refs)
    out_ref = refs.pop()
    values = [[[refs.pop(0)[...] for _ in range(groups)] for groups in shape] for _ in range(1 + exact)]
    high = [refs.pop(0) for _ in shape]
    low = [refs.pop(0) for _ in shape] if exact else None
    total = refs[0][...] if refs else None
    cols = out_ref.shape[0]
    for k in range(len(shape)):
        rows = [group for value in values for group in value[k]]
        term = nn(jnp.concatenate(rows, axis=0) if len(rows) > 1 else rows[0], high[k][...])
        if exact:
            first = values[0][k]
            more = nn(jnp.concatenate(first, axis=0) if len(first) > 1 else first[0], low[k][...])
            term = term[:cols] + (term[cols:] + more)
        total = term if total is None else total + term
    out_ref[...] = total


def apply(values, high, low, where, total):
    depth = values[0][0][0].shape[1]
    cols = sum(group.shape[0] for group in values[0][0])
    rows = high.shape[1]
    tile = tile_of(rows)
    shape = [len(piece) for piece in values[0]]
    count = len(shape)
    exact = len(values) > 1
    flat = [group for value in values for piece in value for group in piece]
    more = [] if total is None else [total]
    matrix = [pl.BlockSpec((depth, tile), functools.partial(lambda p, r, where: (where[p], r), p)) for p in range(count)]
    in_specs = [pl.BlockSpec(group.shape, lambda r, where: (0, 0)) for group in flat]
    in_specs += matrix * (1 + exact)
    in_specs += [pl.BlockSpec((cols, tile), lambda r, where: (0, r)) for _ in more]
    return pl.pallas_call(
        functools.partial(apply_kernel, shape, exact),
        grid_spec=pltpu.PrefetchScalarGridSpec(
            num_scalar_prefetch=1,
            grid=(rows // tile,),
            in_specs=in_specs,
            out_specs=pl.BlockSpec((cols, tile), lambda r, where: (0, r)),
        ),
        out_shape=jax.ShapeDtypeStruct((cols, rows), f32),
        cost_estimate=pl.CostEstimate(
            flops=(6 if exact else 2) * count * cols * depth * rows, bytes_accessed=6 * count * depth * rows, transcendentals=0
        ),
        name="apply",
    )(where, *flat, *([high] * count), *([low] * count if exact else []), *more)


def local(n_silo, n_row, silo_grams, silo_weights):
    return merge(n_silo, n_row, silo_grams, silo_weights)


def merge(n_silo, n_row, silo_grams, silo_weights):
    silos, rows, width = silo_grams.shape
    cols = silo_weights.shape[2]
    mine = cols // n_silo
    served = mine // n_row
    small = mine // CHUNKS
    silo, row = lax.axis_index("silo"), lax.axis_index("row")

    offsets = sorted(range(0, n_row, 2), key=lambda j: (bin(j).count("1"), j))
    final = offsets[-1]
    early = [j for j in offsets if j != final]

    def where(js):
        return row ^ jnp.array(js, jnp.int32)

    def hops(j):
        bits = [1 << k for k in range(1, n_row.bit_length()) if j >> k & 1]
        return bits[-1], bits[0]

    def gather_halves(halves):
        held = {0: list(halves)}
        for j in offsets[1:]:
            held[j] = []
            for p, hop in enumerate(hops(j)[: len(halves)]):
                held[j].append(swap(held[j ^ hop][p], "row", n_row, hop))
        return held

    def gather_rows(value):
        size = value.shape[0] // 2
        held = {0: [value]}

        def part(j, p):
            return held[j][p] if len(held[j]) == 2 else held[j][0][p * size : (p + 1) * size]

        for j in offsets[1:]:
            far, near = hops(j)
            if far == near:
                held[j] = [swap(value, "row", n_row, far)]
            else:
                held[j] = [swap(part(j ^ hop, p), "row", n_row, hop) for p, hop in enumerate((far, near))]
        return held

    def cross(value):
        return swap(value, "row", n_row, 1)

    def sum_silos(pieces):
        return sum((swap(pieces[j], "silo", n_silo, j) for j in range(1, n_silo)), pieces[0])

    def gather_silos(value):
        return jnp.concatenate([value] + [swap(value, "silo", n_silo, j) for j in range(1, n_silo)])

    half = silos // 2 if silos % 2 == 0 else silos
    held = gather_halves([silo_weights[i : i + half] for i in range(0, silos, half)])
    crossed = {j: [cross(x) for x in held[j]] for j in offsets}

    high, low, sums, diag = prepare(silo_grams, row)
    top = jnp.max(jnp.abs(silo_weights.astype(f32)))
    facts = jnp.stack([diag[:, 0], sums[:, 0], jnp.full((rows,), top)])
    others = [facts] + [swap(facts, "silo", n_silo, j) for j in range(1, n_silo)]
    diag = sum(o[0] for o in others)
    reach = jnp.max(sum(o[1] for o in others))
    top = functools.reduce(jnp.maximum, [o[2, 0] for o in others])
    lane = lax.broadcasted_iota(jnp.int32, (n_row, 128), 1)
    slot = lax.broadcasted_iota(jnp.int32, (n_row, 128), 0)
    entry = jnp.where(lane == 0, jnp.sum(diag * diag), jnp.where(lane == 1, jnp.sum(diag * diag * diag), jnp.where(lane == 2, reach, top)))
    table = lax.psum(jnp.where(slot == row, entry, 0.0), "row")
    shift = jnp.sum(table[:, 0]) / jnp.sum(table[:, 1])
    reach, top = jnp.max(table[:, 2]), jnp.max(table[:, 3])
    b_scale = 32768.0 / (reach * top)

    total = rhs([held[j] for j in early], silo_grams, where(early), None, False)
    total = rhs([crossed[j] for j in early], silo_grams, where([j ^ 1 for j in early]), total, False)
    total = rhs([held[final], crossed[final]], silo_grams, where([final, final ^ 1]), total, True)
    total = total.reshape(n_silo, CHUNKS, small, rows)
    b = [
        sum_silos([lax.dynamic_index_in_dim(total, silo ^ j, axis=0, keepdims=False)[c] for j in range(n_silo)])
        for c in range(CHUNKS)
    ]

    def multiply(values, low):
        crossed = [{j: [cross(x) for x in piece] for j, piece in held.items()} for held in values]
        both = [{**held, **{j ^ 1: piece for j, piece in other.items()}} for held, other in zip(values, crossed)]
        total = None
        for js in (early, [j ^ 1 for j in early], [final, final ^ 1]):
            total = apply([[x[j] for j in js] for x in both], high, low, where(js), total)
        return total

    def q_of(exact):
        sent = lax.reduce_precision(exact * b_scale, 5, 10)
        held = gather_rows(gather_silos(sent.astype(f16)))
        held = {j: [split(x.astype(f32)) for x in piece] for j, piece in held.items()}
        total = multiply([{j: [x[i] for x in piece] for j, piece in held.items()} for i in range(2)], low)
        lost = exact - sent / b_scale
        return sum_silos(list(total.reshape(n_silo, small, rows))) / b_scale + diag[None] * lost

    q = [q_of(x) for x in b]

    def curve_of(x, y):
        upper, lower = split(x - shift * y)
        upper, lower = gather_silos(upper), gather_silos(lower)
        total = multiply([gather_rows(upper)], None)
        return jnp.sum(total * (upper.astype(f32) + 2.0 * lower.astype(f32)), axis=1).reshape(n_silo, small)

    curved = jnp.concatenate([curve_of(x, y) for x, y in zip(b, q)], axis=1)
    curved = jnp.stack([lax.dynamic_index_in_dim(curved, silo ^ j, axis=0, keepdims=False) for j in range(n_silo)])
    curved = lax.all_to_all(curved.reshape(n_silo * n_row, served), ("silo", "row"), split_axis=0, concat_axis=0, tiled=True)
    vav = jnp.sum(curved, axis=0)

    both = jnp.stack([jnp.concatenate(b), jnp.concatenate(q)]).reshape(2, n_row, served, rows)
    both = lax.all_to_all(both, "row", split_axis=1, concat_axis=1, tiled=True)
    bt, qt = (jnp.swapaxes(x, 0, 1).reshape(served, width) for x in both)
    bb, bq, qq = (jnp.sum(x, axis=1) for x in (bt * bt, bt * qt, qt * qt))
    first = bb / bq
    next_norm = bb - 2.0 * first * bq + first * first * qq
    beta = next_norm / bb
    nu = first / shift
    mu = 1.0 + beta - nu
    curvature = mu * mu * bq + 2.0 * mu * nu * (bq - shift * qq) + nu * nu * vav
    second = next_norm / curvature
    return (first + second * (1.0 + beta))[:, None] * bt - (second * first)[:, None] * qt


def solution(mesh):
    placed = (P("silo", "row", None), P("silo", "row", None))
    body = functools.partial(local, mesh.shape["silo"], mesh.shape["row"])
    return jax.shard_map(body, mesh=mesh, in_specs=placed, out_specs=P(("silo", "row"), None), check_vma=False)
```

```python
import functools

import jax
import jax.numpy as jnp
from jax import lax
from jax.experimental import pallas as pl
from jax.experimental.pallas import tpu as pltpu
from jax.sharding import PartitionSpec as P


f32, bf16, f16 = jnp.float32, jnp.bfloat16, jnp.float16
CHUNKS = 1


def swap(value, axis, size, bit):
    return lax.ppermute(value, axis, [(i, i ^ bit) for i in range(size)])


def split(value):
    high = lax.reduce_precision(value, 8, 7)
    return high.astype(bf16), (value - high).astype(bf16)


def split_here(value):
    high = value.astype(bf16)
    return high, (value - high.astype(f32)).astype(bf16)


def nn(left, right):
    return lax.dot_general(left, right, (((1,), (0,)), ((), ())), preferred_element_type=f32)


def tile_of(rows):
    return 256 if rows % 256 == 0 else rows


def prepare_kernel(row_ref, gram_ref, weight_ref, high_ref, low_ref, facts_ref):
    block = pl.program_id(0)
    rows = gram_ref.shape[1]
    total = jnp.sum(gram_ref[...], axis=0).T
    high, low = split_here(total)
    high_ref[...] = high
    low_ref[...] = low
    sizes = jnp.sum(jnp.abs(gram_ref[...]), axis=0).astype(bf16)
    ones = jnp.ones((facts_ref.shape[0], rows), bf16)
    sums = lax.dot_general(ones, sizes, (((1,), (1,)), ((), ())), preferred_element_type=f32)
    place = lax.broadcasted_iota(jnp.int32, facts_ref.shape, 0)

    @pl.when(block == 0)
    def _():
        top = jnp.max(jnp.abs(weight_ref[...].astype(f32)))
        facts_ref[...] = jnp.where(place == 2, top / rows, 0.0)

    facts_ref[...] += jnp.where(place == 1, sums, 0.0)

    @pl.when(block == row_ref[0])
    def _():
        here = lax.broadcasted_iota(jnp.int32, (rows, rows), 0)
        there = lax.broadcasted_iota(jnp.int32, (rows, rows), 1)
        diag = jnp.sum(jnp.where(here == there, total, 0.0), axis=0, keepdims=True)
        facts_ref[...] += jnp.where(place == 0, diag, 0.0)


def prepare(grams, weights, row):
    silos, rows, width = grams.shape
    shape = jax.ShapeDtypeStruct
    return pl.pallas_call(
        prepare_kernel,
        grid_spec=pltpu.PrefetchScalarGridSpec(
            num_scalar_prefetch=1,
            grid=(width // rows,),
            in_specs=[
                pl.BlockSpec((silos, rows, rows), lambda k, row: (0, 0, k)),
                pl.BlockSpec(weights.shape, lambda k, row: (0, 0, 0)),
            ],
            out_specs=[
                pl.BlockSpec((rows, rows), lambda k, row: (k, 0)),
                pl.BlockSpec((rows, rows), lambda k, row: (k, 0)),
                pl.BlockSpec((8, rows), lambda k, row: (0, 0)),
            ],
        ),
        out_shape=[shape((width, rows), bf16), shape((width, rows), bf16), shape((8, rows), f32)],
        cost_estimate=pl.CostEstimate(flops=400 * grams.size, bytes_accessed=6 * grams.size, transcendentals=0),
        name="prepare",
    )(row[None], grams, weights)


def rhs_kernel(count, parts, last, where_ref, *refs):
    grams, weights, rest = refs[:count], refs[count : count * (1 + parts)], refs[count * (1 + parts) :]
    out_ref = rest[-1]
    total = rest[0][...] if len(rest) > 1 else None
    left, right = [], []
    for k in range(count):
        each = grams[k].shape[0] // parts
        for i in range(grams[k].shape[0]):
            left += split_here(grams[k][i])
            right += [weights[k * parts + i // each][i % each]] * 2
    term = nn(jnp.concatenate(left, axis=1), jnp.concatenate(right, axis=0))
    total = term if total is None else total + term
    out_ref[...] = total.T if last else total


def rhs(pieces, grams, where, total, last):
    silos, rows, _ = grams.shape
    parts = len(pieces[0])
    depth, cols = pieces[0][0].shape[1:]
    tile = tile_of(rows)
    count = len(pieces)
    flat = [half for piece in pieces for half in piece]
    more = [] if total is None else [total]
    in_specs = [pl.BlockSpec((silos, tile, depth), functools.partial(lambda p, r, where: (0, r, where[p]), p)) for p in range(count)]
    in_specs += [pl.BlockSpec(memory_space=pltpu.VMEM)] * len(flat)
    in_specs += [pl.BlockSpec((tile, cols), lambda r, where: (r, 0)) for _ in more]
    return pl.pallas_call(
        functools.partial(rhs_kernel, count, parts, last),
        grid_spec=pltpu.PrefetchScalarGridSpec(
            num_scalar_prefetch=1,
            grid=(rows // tile,),
            in_specs=in_specs,
            out_specs=pl.BlockSpec((cols, tile), lambda r, where: (0, r)) if last else pl.BlockSpec((tile, cols), lambda r, where: (r, 0)),
        ),
        out_shape=jax.ShapeDtypeStruct((cols, rows) if last else (rows, cols), f32),
        cost_estimate=pl.CostEstimate(
            flops=8 * count * silos * rows * depth * cols, bytes_accessed=4 * count * silos * rows * depth, transcendentals=0
        ),
        name="rhs",
    )(where, *([grams] * count), *flat, *more)


def apply_kernel(shape, exact, where_ref, *refs):
    refs = list(refs)
    out_ref = refs.pop()
    values = [[[refs.pop(0)[...] for _ in range(groups)] for groups in shape] for _ in range(1 + exact)]
    high = [refs.pop(0) for _ in shape]
    low = [refs.pop(0) for _ in shape] if exact else None
    total = refs[0][...] if refs else None
    left, right = [], []
    for k in range(len(shape)):
        rows = [value[k][0] if len(value[k]) == 1 else jnp.concatenate(value[k], axis=0) for value in values]
        left += rows + rows[: 1 if exact else 0]
        right += [high[k][...]] * len(rows) + ([low[k][...]] if exact else [])
    term = nn(left[0], right[0]) if len(left) == 1 else nn(jnp.concatenate(left, axis=1), jnp.concatenate(right, axis=0))
    out_ref[...] = term if total is None else total + term


def apply(values, high, low, where, total):
    depth = values[0][0][0].shape[1]
    cols = sum(group.shape[0] for group in values[0][0])
    rows = high.shape[1]
    tile = tile_of(rows)
    shape = [len(piece) for piece in values[0]]
    count = len(shape)
    exact = len(values) > 1
    flat = [group for value in values for piece in value for group in piece]
    more = [] if total is None else [total]
    matrix = [pl.BlockSpec((depth, tile), functools.partial(lambda p, r, where: (where[p], r), p)) for p in range(count)]
    in_specs = [pl.BlockSpec(memory_space=pltpu.VMEM)] * len(flat)
    in_specs += matrix * (1 + exact)
    in_specs += [pl.BlockSpec((cols, tile), lambda r, where: (0, r)) for _ in more]
    return pl.pallas_call(
        functools.partial(apply_kernel, shape, exact),
        grid_spec=pltpu.PrefetchScalarGridSpec(
            num_scalar_prefetch=1,
            grid=(rows // tile,),
            in_specs=in_specs,
            out_specs=pl.BlockSpec((cols, tile), lambda r, where: (0, r)),
        ),
        out_shape=jax.ShapeDtypeStruct((cols, rows), f32),
        cost_estimate=pl.CostEstimate(
            flops=(6 if exact else 2) * count * cols * depth * rows, bytes_accessed=6 * count * depth * rows, transcendentals=0
        ),
        name="apply",
    )(where, *flat, *([high] * count), *([low] * count if exact else []), *more)


def local(n_silo, n_row, silo_grams, silo_weights):
    return merge(n_silo, n_row, silo_grams, silo_weights)


def merge(n_silo, n_row, silo_grams, silo_weights):
    silos, rows, width = silo_grams.shape
    cols = silo_weights.shape[2]
    mine = cols // n_silo
    served = mine // n_row
    small = mine // CHUNKS
    silo, row = lax.axis_index("silo"), lax.axis_index("row")

    offsets = sorted(range(0, n_row, 2), key=lambda j: (bin(j).count("1"), j))
    levels = {}
    for j in offsets:
        levels.setdefault(bin(j).count("1"), []).extend([j, j ^ 1])
    levels = [levels[k] for k in sorted(levels)]

    def where(js):
        return row ^ jnp.array(js, jnp.int32)

    def hops(j):
        bits = [1 << k for k in range(1, n_row.bit_length()) if j >> k & 1]
        return bits[-1], bits[0]

    def gather_halves(halves):
        held = {0: list(halves)}
        for j in offsets[1:]:
            held[j] = []
            for p, hop in enumerate(hops(j)[: len(halves)]):
                held[j].append(swap(held[j ^ hop][p], "row", n_row, hop))
        return held

    def cross(value):
        return swap(value, "row", n_row, 1)

    def sum_silos(pieces):
        return sum((swap(pieces[j], "silo", n_silo, j) for j in range(1, n_silo)), pieces[0])

    def gather_silos(value):
        held = [value]
        for j in range(1, n_silo):
            held.append(swap(value, "silo", n_silo, j))
        return [jnp.concatenate(held[: n_silo // 2]), jnp.concatenate(held[n_silo // 2 :])]

    half = silos // 2 if silos % 2 == 0 else silos
    held = gather_halves([silo_weights[i : i + half] for i in range(0, silos, half)])
    crossed = {j: [cross(x) for x in held[j]] for j in offsets}

    high, low, facts = prepare(silo_grams, silo_weights, row)
    others = [facts]
    for j in range(1, n_silo):
        others.append(swap(facts, "silo", n_silo, j))
    facts = sum(others)
    diag = facts[0]
    place = lax.broadcasted_iota(jnp.int32, facts.shape, 0)
    facts = jnp.where(place == 0, diag * diag, jnp.where(place == 3, diag * diag * diag, facts))
    facts = jnp.sum(facts, axis=1)
    held.update({j ^ 1: piece for j, piece in crossed.items()})
    total = None
    for k, js in enumerate(levels):
        total = rhs([held[j] for j in js], silo_grams, where(js), total, js is levels[-1])
        if k == 0:
            total, diag, facts = lax.optimization_barrier((total, diag, facts))
    slot = lax.broadcasted_iota(jnp.int32, (n_row, 8), 0)
    table = lax.psum(jnp.where(slot == row, facts[None], 0.0), "row")
    shift = jnp.sum(table[:, 0]) / jnp.sum(table[:, 3])
    reach = 1.01 * jnp.max(table[:, 1])
    top = jnp.max(table[:, 2])
    b_scale = 32768.0 / (reach * top)

    total = total.reshape(n_silo, CHUNKS, small, rows)
    b = [
        sum_silos([lax.dynamic_index_in_dim(total, silo ^ j, axis=0, keepdims=False)[c] for j in range(n_silo)])
        for c in range(CHUNKS)
    ]

    def multiply(values, low):
        crossed = [{j: [cross(x) for x in piece] for j, piece in held.items()} for held in values]
        both = [{**held, **{j ^ 1: piece for j, piece in other.items()}} for held, other in zip(values, crossed)]
        total = None
        for js in levels:
            before = total
            total = apply([[x[j] for j in js] for x in both], high, low, where(js), total)
        return before, total

    def q_of(exact):
        sent = lax.reduce_precision(exact * b_scale, 5, 10)
        held = gather_halves(gather_silos(sent.astype(f16)))
        for piece in held.values():
            for p, x in enumerate(piece):
                piece[p] = split(x.astype(f32))
        _, total = multiply([{j: [x[i] for x in piece] for j, piece in held.items()} for i in range(2)], low)
        lost = exact - sent / b_scale
        return sum_silos(list(total.reshape(n_silo, small, rows))) / b_scale + diag[None] * lost

    q = [q_of(x) for x in b]

    def curve_of(x, y):
        upper, lower = split(x - shift * y)
        upper, lower = gather_silos(upper), gather_silos(lower)
        held = gather_halves(upper)
        before = [held[j][0][:8, :128] for j in offsets if bin(j).count("1") == 1]
        _, total = multiply([held], None)
        rounded = jnp.concatenate(upper).astype(f32) + 2.0 * jnp.concatenate(lower).astype(f32)
        return before, jnp.sum(total * rounded, axis=1).reshape(n_silo, small)

    curves = [curve_of(x, y) for x, y in zip(b, q)]
    curved = jnp.concatenate([curve for _, curve in curves], axis=1)
    curved = jnp.stack([lax.dynamic_index_in_dim(curved, silo ^ j, axis=0, keepdims=False) for j in range(n_silo)])
    both = jnp.stack([jnp.concatenate(b), jnp.concatenate(q)]).reshape(2, n_row, served, rows)
    both, _ = lax.optimization_barrier((both, curves[-1][0]))
    both = lax.all_to_all(both, "row", split_axis=1, concat_axis=1, tiled=True)
    both, curved = lax.optimization_barrier((both, curved))
    curved = lax.all_to_all(curved.reshape(n_silo * n_row, served), ("silo", "row"), split_axis=0, concat_axis=0, tiled=True)
    vav = jnp.sum(curved, axis=0)
    bt, qt = (jnp.swapaxes(x, 0, 1).reshape(served, width) for x in both)
    bb, bq, qq = (jnp.sum(x, axis=1) for x in (bt * bt, bt * qt, qt * qt))
    first = bb / bq
    next_norm = bb - 2.0 * first * bq + first * first * qq
    beta = next_norm / bb
    nu = first / shift
    mu = 1.0 + beta - nu
    curvature = mu * mu * bq + 2.0 * mu * nu * (bq - shift * qq) + nu * nu * vav
    second = next_norm / curvature
    return (first + second * (1.0 + beta))[:, None] * bt - (second * first)[:, None] * qt


def solution(mesh):
    placed = (P("silo", "row", None), P("silo", "row", None))
    body = functools.partial(local, mesh.shape["silo"], mesh.shape["row"])
    return jax.shard_map(body, mesh=mesh, in_specs=placed, out_specs=P(("silo", "row"), None), check_vma=False)
```

```python
import functools

import jax
import jax.numpy as jnp
from jax import lax
from jax.experimental import pallas as pl
from jax.experimental.pallas import tpu as pltpu
from jax.sharding import PartitionSpec as P


f32, bf16, f16 = jnp.float32, jnp.bfloat16, jnp.float16
CHUNKS = 1


def swap(value, axis, size, bit):
    return lax.ppermute(value, axis, [(i, i ^ bit) for i in range(size)])


def split(value):
    high = lax.reduce_precision(value, 8, 7)
    return high.astype(bf16), (value - high).astype(bf16)


def split_here(value):
    high = value.astype(bf16)
    return high, (value - high.astype(f32)).astype(bf16)


def nn(left, right):
    return lax.dot_general(left, right, (((1,), (0,)), ((), ())), preferred_element_type=f32)


def tile_of(rows):
    return 256 if rows % 256 == 0 else rows


def prepare_kernel(row_ref, gram_ref, weight_ref, high_ref, low_ref, facts_ref):
    block = pl.program_id(0)
    rows = gram_ref.shape[1]
    total = jnp.sum(gram_ref[...], axis=0).T
    high, low = split_here(total)
    high_ref[...] = high
    low_ref[...] = low
    sizes = jnp.sum(jnp.abs(gram_ref[...]), axis=0).astype(bf16)
    ones = jnp.ones((facts_ref.shape[0], rows), bf16)
    sums = lax.dot_general(ones, sizes, (((1,), (1,)), ((), ())), preferred_element_type=f32)
    place = lax.broadcasted_iota(jnp.int32, facts_ref.shape, 0)

    @pl.when(block == 0)
    def _():
        top = jnp.max(jnp.abs(weight_ref[...].astype(f32)))
        facts_ref[...] = jnp.where(place == 2, top / rows, 0.0)

    facts_ref[...] += jnp.where(place == 1, sums, 0.0)

    @pl.when(block == row_ref[0])
    def _():
        here = lax.broadcasted_iota(jnp.int32, (rows, rows), 0)
        there = lax.broadcasted_iota(jnp.int32, (rows, rows), 1)
        diag = jnp.sum(jnp.where(here == there, total, 0.0), axis=0, keepdims=True)
        facts_ref[...] += jnp.where(place == 0, diag, 0.0)


def prepare(grams, weights, row):
    silos, rows, width = grams.shape
    shape = jax.ShapeDtypeStruct
    return pl.pallas_call(
        prepare_kernel,
        grid_spec=pltpu.PrefetchScalarGridSpec(
            num_scalar_prefetch=1,
            grid=(width // rows,),
            in_specs=[
                pl.BlockSpec((silos, rows, rows), lambda k, row: (0, 0, k)),
                pl.BlockSpec(weights.shape, lambda k, row: (0, 0, 0)),
            ],
            out_specs=[
                pl.BlockSpec((rows, rows), lambda k, row: (k, 0)),
                pl.BlockSpec((rows, rows), lambda k, row: (k, 0)),
                pl.BlockSpec((8, rows), lambda k, row: (0, 0)),
            ],
        ),
        out_shape=[shape((width, rows), bf16), shape((width, rows), bf16), shape((8, rows), f32)],
        cost_estimate=pl.CostEstimate(flops=400 * grams.size, bytes_accessed=6 * grams.size, transcendentals=0),
        name="prepare",
    )(row[None], grams, weights)


def rhs_kernel(count, parts, last, where_ref, *refs):
    grams, weights, rest = refs[:count], refs[count : count * (1 + parts)], refs[count * (1 + parts) :]
    out_ref = rest[-1]
    total = rest[0][...] if len(rest) > 1 else None
    left, right = [], []
    for k in range(count):
        each = grams[k].shape[0] // parts
        for i in range(grams[k].shape[0]):
            left += split_here(grams[k][i])
            right += [weights[k * parts + i // each][i % each]] * 2
    term = nn(jnp.concatenate(left, axis=1), jnp.concatenate(right, axis=0))
    total = term if total is None else total + term
    out_ref[...] = total.T if last else total


def rhs(pieces, grams, where, total, last):
    silos, rows, _ = grams.shape
    parts = len(pieces[0])
    depth, cols = pieces[0][0].shape[1:]
    tile = tile_of(rows)
    count = len(pieces)
    flat = [half for piece in pieces for half in piece]
    more = [] if total is None else [total]
    in_specs = [pl.BlockSpec((silos, tile, depth), functools.partial(lambda p, r, where: (0, r, where[p]), p)) for p in range(count)]
    in_specs += [pl.BlockSpec(memory_space=pltpu.VMEM)] * len(flat)
    in_specs += [pl.BlockSpec((tile, cols), lambda r, where: (r, 0)) for _ in more]
    return pl.pallas_call(
        functools.partial(rhs_kernel, count, parts, last),
        grid_spec=pltpu.PrefetchScalarGridSpec(
            num_scalar_prefetch=1,
            grid=(rows // tile,),
            in_specs=in_specs,
            out_specs=pl.BlockSpec((cols, tile), lambda r, where: (0, r)) if last else pl.BlockSpec((tile, cols), lambda r, where: (r, 0)),
        ),
        out_shape=jax.ShapeDtypeStruct((cols, rows) if last else (rows, cols), f32),
        cost_estimate=pl.CostEstimate(
            flops=8 * count * silos * rows * depth * cols, bytes_accessed=4 * count * silos * rows * depth, transcendentals=0
        ),
        name="rhs",
    )(where, *([grams] * count), *flat, *more)


def apply_kernel(shape, exact, where_ref, *refs):
    refs = list(refs)
    out_ref = refs.pop()
    values = [[[refs.pop(0)[...] for _ in range(groups)] for groups in shape] for _ in range(1 + exact)]
    high = [refs.pop(0) for _ in shape]
    low = [refs.pop(0) for _ in shape] if exact else None
    total = refs[0][...] if refs else None
    left, right = [], []
    for k in range(len(shape)):
        rows = [value[k][0] if len(value[k]) == 1 else jnp.concatenate(value[k], axis=0) for value in values]
        left += rows + rows[: 1 if exact else 0]
        right += [high[k][...]] * len(rows) + ([low[k][...]] if exact else [])
    term = nn(left[0], right[0]) if len(left) == 1 else nn(jnp.concatenate(left, axis=1), jnp.concatenate(right, axis=0))
    out_ref[...] = term if total is None else total + term


def apply(values, high, low, where, total):
    depth = values[0][0][0].shape[1]
    cols = sum(group.shape[0] for group in values[0][0])
    rows = high.shape[1]
    tile = tile_of(rows)
    shape = [len(piece) for piece in values[0]]
    count = len(shape)
    exact = len(values) > 1
    flat = [group for value in values for piece in value for group in piece]
    more = [] if total is None else [total]
    matrix = [pl.BlockSpec((depth, tile), functools.partial(lambda p, r, where: (where[p], r), p)) for p in range(count)]
    in_specs = [pl.BlockSpec(memory_space=pltpu.VMEM)] * len(flat)
    in_specs += matrix * (1 + exact)
    in_specs += [pl.BlockSpec((cols, tile), lambda r, where: (0, r)) for _ in more]
    return pl.pallas_call(
        functools.partial(apply_kernel, shape, exact),
        grid_spec=pltpu.PrefetchScalarGridSpec(
            num_scalar_prefetch=1,
            grid=(rows // tile,),
            in_specs=in_specs,
            out_specs=pl.BlockSpec((cols, tile), lambda r, where: (0, r)),
        ),
        out_shape=jax.ShapeDtypeStruct((cols, rows), f32),
        cost_estimate=pl.CostEstimate(
            flops=(6 if exact else 2) * count * cols * depth * rows, bytes_accessed=6 * count * depth * rows, transcendentals=0
        ),
        name="apply",
    )(where, *flat, *([high] * count), *([low] * count if exact else []), *more)


def local(n_silo, n_row, silo_grams, silo_weights):
    return merge(n_silo, n_row, silo_grams, silo_weights)


def merge(n_silo, n_row, silo_grams, silo_weights):
    silos, rows, width = silo_grams.shape
    cols = silo_weights.shape[2]
    mine = cols // n_silo
    served = mine // n_row
    small = mine // CHUNKS
    silo, row = lax.axis_index("silo"), lax.axis_index("row")

    offsets = sorted(range(0, n_row, 2), key=lambda j: (bin(j).count("1"), j))
    levels = {}
    for j in offsets:
        levels.setdefault(bin(j).count("1"), []).extend([j, j ^ 1])
    levels = [levels[k] for k in sorted(levels)]

    def where(js):
        return row ^ jnp.array(js, jnp.int32)

    def hops(j):
        bits = [1 << k for k in range(1, n_row.bit_length()) if j >> k & 1]
        return bits[-1], bits[0]

    def gather_halves(halves):
        held = {0: list(halves)}
        for j in offsets[1:]:
            held[j] = []
            for p, hop in enumerate(hops(j)[: len(halves)]):
                held[j].append(swap(held[j ^ hop][p], "row", n_row, hop))
        return held

    def cross(value):
        return swap(value, "row", n_row, 1)

    def sum_silos(pieces):
        return sum((swap(pieces[j], "silo", n_silo, j) for j in range(1, n_silo)), pieces[0])

    def gather_silos(value):
        held = [value]
        for j in range(1, n_silo):
            held.append(swap(value, "silo", n_silo, j))
        return [jnp.concatenate(held[: n_silo // 2]), jnp.concatenate(held[n_silo // 2 :])]

    half = silos // 2 if silos % 2 == 0 else silos
    held = gather_halves([silo_weights[i : i + half] for i in range(0, silos, half)])
    crossed = {j: [cross(x) for x in held[j]] for j in offsets}

    high, low, facts = prepare(silo_grams, silo_weights, row)
    others = [facts]
    for j in range(1, n_silo):
        others.append(swap(facts, "silo", n_silo, j))
    facts = sum(others)
    diag = facts[0]
    place = lax.broadcasted_iota(jnp.int32, facts.shape, 0)
    reach = jnp.max(facts[1])
    facts = jnp.where(place == 0, diag * diag, jnp.where(place == 3, diag * diag * diag, facts))
    facts = jnp.sum(facts, axis=1)
    facts = jnp.where(lax.iota(jnp.int32, facts.shape[0]) == 1, reach, facts)
    held.update({j ^ 1: piece for j, piece in crossed.items()})
    total = None
    for k, js in enumerate(levels):
        total = rhs([held[j] for j in js], silo_grams, where(js), total, js is levels[-1])
        if k == 0:
            total, diag, facts = lax.optimization_barrier((total, diag, facts))
    slot = lax.broadcasted_iota(jnp.int32, (n_row, 8), 0)
    table = lax.psum(jnp.where(slot == row, facts[None], 0.0), "row")
    shift = jnp.sum(table[:, 0]) / jnp.sum(table[:, 3])
    reach = 1.01 * jnp.max(table[:, 1])
    top = jnp.max(table[:, 2])
    b_scale = 32768.0 / (reach * top)

    total = total.reshape(n_silo, CHUNKS, small, rows)
    b = [
        sum_silos([lax.dynamic_index_in_dim(total, silo ^ j, axis=0, keepdims=False)[c] for j in range(n_silo)])
        for c in range(CHUNKS)
    ]

    def multiply(values, low):
        crossed = [{j: [cross(x) for x in piece] for j, piece in held.items()} for held in values]
        both = [{**held, **{j ^ 1: piece for j, piece in other.items()}} for held, other in zip(values, crossed)]
        total = None
        for js in levels:
            total = apply([[x[j] for j in js] for x in both], high, low, where(js), total)
        return total

    def q_of(exact):
        sent = lax.reduce_precision(exact * b_scale, 5, 10)
        held = gather_halves(gather_silos(sent.astype(f16)))
        for piece in held.values():
            for p, x in enumerate(piece):
                piece[p] = split(x.astype(f32))
        total = multiply([{j: [x[i] for x in piece] for j, piece in held.items()} for i in range(2)], low)
        lost = exact - sent / b_scale
        total = total.reshape(n_silo, small, rows)
        parts = []
        for j in range(1, n_silo):
            parts.append(swap((total[j] / reach).astype(f16), "silo", n_silo, j))
        return (total[0] + reach * sum(x.astype(f32) for x in parts)) / b_scale + diag[None] * lost

    q = [q_of(x) for x in b]

    def curve_of(x, y):
        upper, lower = split(x - shift * y)
        upper, lower = gather_silos(upper), gather_silos(lower)
        held = gather_halves(upper)
        total = multiply([held], None)
        rounded = jnp.concatenate(upper).astype(f32) + 2.0 * jnp.concatenate(lower).astype(f32)
        return jnp.sum(total * rounded, axis=1).reshape(n_silo, small)

    curves = [curve_of(x, y) for x, y in zip(b, q)]
    curved = jnp.concatenate(curves, axis=1)
    curved = jnp.stack([lax.dynamic_index_in_dim(curved, silo ^ j, axis=0, keepdims=False) for j in range(n_silo)])
    both = []
    for value in (b, q):
        value = jnp.concatenate(value).reshape(n_row, served, rows)
        both.append(lax.all_to_all(value, "row", split_axis=0, concat_axis=0, tiled=True))
    both, curved = lax.optimization_barrier((both, curved))
    curved = lax.all_to_all(curved.reshape(n_silo * n_row, served), ("silo", "row"), split_axis=0, concat_axis=0, tiled=True)
    vav = jnp.sum(curved, axis=0)
    bt, qt = (jnp.swapaxes(x, 0, 1).reshape(served, width) for x in both)
    bb, bq, qq = (jnp.sum(x, axis=1) for x in (bt * bt, bt * qt, qt * qt))
    first = bb / bq
    next_norm = bb - 2.0 * first * bq + first * first * qq
    beta = next_norm / bb
    nu = first / shift
    mu = 1.0 + beta - nu
    curvature = mu * mu * bq + 2.0 * mu * nu * (bq - shift * qq) + nu * nu * vav
    second = next_norm / curvature
    return (first + second * (1.0 + beta))[:, None] * bt - (second * first)[:, None] * qt


def solution(mesh):
    placed = (P("silo", "row", None), P("silo", "row", None))
    body = functools.partial(local, mesh.shape["silo"], mesh.shape["row"])
    return jax.shard_map(body, mesh=mesh, in_specs=placed, out_specs=P(("silo", "row"), None), check_vma=False)
```
